32 devices in a mesh: copy: 4 (over y, x), rows: 2 (over z_hi), cols: 2 (over core), slabs: 2 (over z_lo).
Axes of the slice: x: 2, y: 2, z: 4 (z_hi: 2, z_lo: 2; z = z_hi * 2 + z_lo), core: 2. Of those that a mesh axis runs over, the one named last changes fastest.
Arguments:
- density: float32 [128, 16, 128, 128], P(('copy', 'rows'), 'cols', 'slabs'), parts along dimension 0, may hold values from 0.2 to 1.8
- crowding: float32 [128, 16, 128, 128], P(('copy', 'rows'), 'cols', 'slabs'), parts along dimension 0, may hold values from 0.5 to 2
Outputs:
- potential: float32 [128, 16, 128, 128], P(('copy', 'rows'), 'cols', 'slabs'), parts along dimension 0
- density_end: float32 [128, 16, 128, 128], P(('copy', 'rows'), 'cols', 'slabs'), parts along dimension 0
The draws below stay inside these ranges and needn't reach their ends.
There are 4 independent parts, one for each index of `copy`. The reference program is written for one: setup_inputs(seed, part) draws one part's arguments, and reference() takes and returns one part's arrays. A program takes and returns all parts, laid end to end along the dimension named above; each array names one. Nothing has to cross between parts.
All inputs are finite; a program needn't handle non-finite values.
Results may differ from the reference program's by a relative error of at most 0.00002.
Values sent between devices are 32-bit elements; how exact they have to be, the bound alone decides.
A program may use at most 128 MiB of HBM per device.

```python
import jax
import jax.numpy as jnp
from jax import lax

GRID_J = 32
GRID_I = 16
GRID_K = 128
SPECIES = 128
STEPS = 6


def steps_of(rng, shape, shards, low, high):
    gain = 1.0
    for position, parts in shards:
        draws = jax.random.uniform(jax.random.fold_in(jax.random.fold_in(rng, 6), position), (parts,), jnp.float32, low / len(shards), high / len(shards))
        gain = gain * jnp.repeat(jnp.exp(draws), shape[position] // parts).reshape((-1,) + (1,) * (len(shape) - 1 - position))
    return gain


def setup_inputs(seed: int = 0, part: int = 0) -> dict:
    arg_keys = jax.random.split(jax.random.key(seed), 3)
    part_splits = jax.random.split(jax.random.fold_in(arg_keys[2], part), 3)
    return {
        "density": jnp.clip(0.2 + 1.5999999 * jax.random.uniform(part_splits[0], (GRID_J, GRID_I, GRID_K, SPECIES), jnp.float32) ** steps_of(part_splits[0], (GRID_J, GRID_I, GRID_K, SPECIES), ((0, 2), (1, 2), (2, 2)), -0.2, 0.2), 0.2, 1.8),
        "crowding": jnp.clip(0.5 + 1.5 * jax.random.uniform(part_splits[1], (GRID_J, GRID_I, GRID_K, SPECIES), jnp.float32) ** steps_of(part_splits[1], (GRID_J, GRID_I, GRID_K, SPECIES), ((0, 2), (1, 2), (2, 2)), -0.2, 0.2), 0.5, 2.0),
    }


def strip_edges(values, dims):
    for dim in dims:
        values = lax.slice_in_dim(values, 1, values.shape[dim] - 1, axis=dim)
    return values


def neighbour(values, dim, start, dims):
    others = [other for other in dims if other != dim]
    values = strip_edges(values, others)
    return lax.slice_in_dim(values, start, start + values.shape[dim] - 2, axis=dim)


def one_step(padded, crowding):
    middle = strip_edges(padded, (0, 1, 2))
    lower = [neighbour(padded, dim, 0, (0, 1, 2)) for dim in (0, 1, 2)]
    upper = [neighbour(padded, dim, 2, (0, 1, 2)) for dim in (0, 1, 2)]
    spread = lower[0] + upper[0] + lower[1] + upper[1] + lower[2] + upper[2] - 6.0 * middle
    return middle + 0.1 * spread + 0.2 * middle * (1.0 - middle * crowding)


def reference(density, crowding):
    for step in range(STEPS):
        density = one_step(jnp.pad(density, ((1, 1), (1, 1), (1, 1), (0, 0)), mode="wrap"), crowding)
    potential = jnp.cumsum(density, axis=1) / GRID_I
    return potential, density
```

```python
import functools

import jax
import jax.numpy as jnp
from jax import lax
from jax.experimental import pallas as pl
from jax.experimental.pallas import tpu as pltpu
from jax.sharding import PartitionSpec as P

STEPS = 6
MESH = pl.DeviceIdType.MESH
PAD = 8


def kernel(shape, counts, dens, crow, pot_out, end_out, X, C, PT, KS, KR, TS, TR,
           js, jr, is_, ir, ks, kr, ts, tr, ls):
    J, I, K, S = shape
    n_rows, n_cols, n_slabs = counts
    cells = I * n_cols
    inner = pl.ds(PAD, K)

    def ring(axis, count, offset):
        return {axis: lax.rem(lax.axis_index(axis) + (offset + count), count)}

    load_d = pltpu.make_async_copy(dens, X.at[0, pl.ds(1, J), pl.ds(1, I), inner, :], ls.at[0])
    load_c = pltpu.make_async_copy(crow, C, ls.at[1])
    load_d.start()
    load_c.start()

    barrier = pltpu.get_barrier_semaphore()
    greeted = [ring("rows", n_rows, o) for o in (-1, 1)]
    greeted += [ring("slabs", n_slabs, o) for o in (-1, 1)]
    greeted += [ring("cols", n_cols, o) for o in (-1, 1)]
    greeted += [ring("cols", n_cols, o) for o in range(1, n_cols)]
    for device in greeted:
        pl.semaphore_signal(barrier, inc=1, device_id=device, device_id_type=MESH)
    pl.semaphore_wait(barrier, len(greeted))

    groups = ((1, 1), (2, J - 2), (J, 1))

    def remote(src, dst, send, recv, device):
        return pltpu.make_async_remote_copy(
            src_ref=src, dst_ref=dst, send_sem=send, recv_sem=recv,
            device_id=device, device_id_type=MESH)

    def j_copy(side, b, src=None):
        mine, theirs = ((1, J + 1), (J, 0))[side]
        if src is None:
            src = X.at[b, mine, pl.ds(1, I), inner, :]
        return remote(src, X.at[b, theirs, pl.ds(1, I), inner, :],
                      js.at[side, b], jr.at[side, b], ring("rows", n_rows, (-1, 1)[side]))

    def i_copy(side, g, b):
        mine, theirs = ((1, I + 1), (I, 0))[side]
        first, size = groups[g]
        return remote(X.at[b, pl.ds(first, size), mine, inner, :],
                      X.at[b, pl.ds(first, size), theirs, inner, :],
                      is_.at[side, g, b], ir.at[side, g, b], ring("cols", n_cols, (-1, 1)[side]))

    def k_copy(side, g, b):
        first, size = groups[g]
        return remote(KS.at[b, side, pl.ds(first - 1, size)],
                      KR.at[b, 1 - side, pl.ds(first - 1, size)],
                      ks.at[side, g, b], kr.at[side, g, b], ring("slabs", n_slabs, (-1, 1)[side]))

    def t_copy(offset, g):
        first, size = groups[g]
        return remote(TS.at[pl.ds(first - 1, size)], TR.at[offset - 1, pl.ds(first - 1, size)],
                      ts.at[offset - 1, g], tr.at[offset - 1, g], ring("cols", n_cols, offset))

    ik = lambda g, b: [k_copy(s, g, b) for s in (0, 1)] + [i_copy(s, g, b) for s in (0, 1)]

    def over(g, body):
        first, size = groups[g]

        def at(n, carry):
            body(first + n // I, 1 + n % I)
            return carry

        lax.fori_loop(0, size * I, at, 0)

    def pack(b, j, i, low, high):
        KS[b, 0, j - 1, pl.ds(i - 1, 1), :] = low
        KS[b, 1, j - 1, pl.ds(i - 1, 1), :] = high

    def update(b, g, last):
        nb = 1 - b

        def unpack(j, i):
            X[b, j, i, PAD - 1:PAD, :] = KR[b, 0, j - 1, pl.ds(i - 1, 1), :]
            X[b, j, i, PAD + K:PAD + K + 1, :] = KR[b, 1, j - 1, pl.ds(i - 1, 1), :]

        over(g, unpack)

        def cell(j, i):
            c = X[b, j, i, PAD:PAD + K, :]
            around = X[b, j, i, PAD - 1:PAD + K - 1, :] + X[b, j, i, PAD + 1:PAD + K + 1, :]
            around += X[b, j - 1, i, PAD:PAD + K, :] + X[b, j + 1, i, PAD:PAD + K, :]
            around += X[b, j, i - 1, PAD:PAD + K, :] + X[b, j, i + 1, PAD:PAD + K, :]
            c2 = c * 0.2
            new = 0.1 * around + (c * 0.4 + c2 * (1.0 - c * C[j - 1, i - 1]))
            X[nb, j, i, PAD:PAD + K, :] = new
            if not last:
                pack(nb, j, i, new[:1], new[K - 1:])

        over(g, cell)

    sent_j = {}
    sent_j[0, 0] = j_copy(0, 0, dens.at[0])
    sent_j[0, 0].start()
    load_d.wait()
    for g in range(3):
        over(g, lambda j, i: pack(0, j, i, X[0, j, i, PAD:PAD + 1, :], X[0, j, i, PAD + K - 1:PAD + K, :]))
    sent = {}
    for g in (1, 0, 2):
        sent[0, g] = ik(g, 0)
        for copy in sent[0, g]:
            copy.start()
    sent_j[0, 1] = j_copy(1, 0, dens.at[J - 1])
    sent_j[0, 1].start()
    load_c.wait()

    writes = []
    for t in range(STEPS):
        b, nb, last = t % 2, 1 - t % 2, t == STEPS - 1
        for g in (1, 0, 2):
            for copy in sent[t, g]:
                copy.wait_recv()
            if g != 1:
                side = g // 2
                sent_j[t, 1 - side].wait_recv()
            if t >= 1:
                for copy in sent[t - 1, g]:
                    copy.wait_send()
                if g != 1:
                    sent_j[t - 1, g // 2].wait_send()
            update(b, g, last)
            if not last:
                sent[t + 1, g] = ik(g, nb)
                for copy in sent[t + 1, g]:
                    copy.start()
                if g != 1:
                    sent_j[t + 1, g // 2] = j_copy(g // 2, nb)
                    sent_j[t + 1, g // 2].start()
                continue
            first, size = groups[g]
            write = pltpu.make_async_copy(
                X.at[nb, pl.ds(first, size), pl.ds(1, I), inner, :],
                end_out.at[pl.ds(first - 1, size)], ls.at[2 + g])
            write.start()
            writes.append(write)

            def total(n, carry, first=first):
                j = first + n
                so_far = X[nb, j, 1, PAD:PAD + K, :]
                for i in range(2, I + 1):
                    so_far += X[nb, j, i, PAD:PAD + K, :]
                TS[j - 1] = so_far
                return carry

            lax.fori_loop(0, size, total, 0)
            copies = [t_copy(o, g) for o in range(1, n_cols)]
            for copy in copies:
                copy.start()
            for copy in copies:
                copy.wait()
            me = lax.axis_index("cols")

            def running(n, carry, first=first):
                j = first + n
                so_far = jnp.zeros((K, S), jnp.float32)
                for o in range(1, n_cols):
                    so_far += jnp.where(o <= me, TR[o - 1, j - 1], 0.0)
                for i in range(1, I + 1):
                    so_far += X[nb, j, i, PAD:PAD + K, :]
                    PT[j - 1, i - 1] = so_far * (1.0 / cells)
                return carry

            lax.fori_loop(0, size, running, 0)
            write = pltpu.make_async_copy(
                PT.at[pl.ds(first - 1, size)], pot_out.at[pl.ds(first - 1, size)], ls.at[5 + g])
            write.start()
            writes.append(write)
    for g in range(3):
        for copy in sent[STEPS - 1, g]:
            copy.wait_send()
    for side in range(2):
        sent_j[STEPS - 1, side].wait_send()
    for write in writes:
        write.wait()


def solution(mesh):
    counts = tuple(mesh.shape[axis] for axis in ("rows", "cols", "slabs"))

    def per_device(density, crowding):
        J, I, K, S = density.shape
        n_cols = counts[1]
        any_space = pl.BlockSpec(memory_space=pl.ANY)
        dma = pltpu.SemaphoreType.DMA
        return pl.pallas_call(
            functools.partial(kernel, density.shape, counts),
            out_shape=[jax.ShapeDtypeStruct(density.shape, density.dtype)] * 2,
            in_specs=[any_space] * 2,
            out_specs=[any_space] * 2,
            scratch_shapes=[
                pltpu.VMEM((2, J + 2, I + 2, K + 2 * PAD, S), jnp.float32),
                pltpu.VMEM((J, I, K, S), jnp.float32),
                pltpu.VMEM((J, I, K, S), jnp.float32),
                pltpu.VMEM((2, 2, J, I, S), jnp.float32),
                pltpu.VMEM((2, 2, J, I, S), jnp.float32),
                pltpu.VMEM((J, K, S), jnp.float32),
                pltpu.VMEM((n_cols - 1, J, K, S), jnp.float32),
                dma((2, 2)), dma((2, 2)),
                dma((2, 3, 2)), dma((2, 3, 2)),
                dma((2, 3, 2)), dma((2, 3, 2)),
                dma((n_cols - 1, 3)), dma((n_cols - 1, 3)),
                dma((8,)),
            ],
            compiler_params=pltpu.CompilerParams(
                collective_id=0, has_side_effects=True, vmem_limit_bytes=56 * 2**20),
            name="reaction_diffusion",
        )(density, crowding)

    spec = P(("copy", "rows"), "cols", "slabs", None)
    return jax.shard_map(
        per_device, mesh=mesh, in_specs=(spec, spec), out_specs=(spec, spec), check_vma=False)
```

```python
import functools

import jax
import jax.numpy as jnp
from jax import lax
from jax.experimental import pallas as pl
from jax.experimental.pallas import tpu as pltpu
from jax.sharding import PartitionSpec as P

STEPS = 6
MESH = pl.DeviceIdType.MESH
VMEM_FIRST = 47 * 2**20
VMEM_SECOND = 20 * 2**20
PAD = 8


def kernel(shape, counts, dens, crow, end, below, X0, X1, C, KS, KR, TS, TR,
           js, jr, is_, ir, ks, kr, ts, tr, ls):
    J, I, K, S = shape
    n_rows, n_cols, n_slabs = counts
    X = (X0, X1)
    inner = pl.ds(PAD, K)

    def ring(axis, count, offset):
        return {axis: lax.rem(lax.axis_index(axis) + (offset + count), count)}

    load_d = pltpu.make_async_copy(dens, X0.at[pl.ds(1, J), pl.ds(1, I), inner, :], ls.at[0])
    load_c = pltpu.make_async_copy(crow, C, ls.at[1])
    load_d.start()
    load_c.start()

    barrier = pltpu.get_barrier_semaphore()
    greeted = [ring("rows", n_rows, o) for o in (-1, 1)]
    greeted += [ring("slabs", n_slabs, o) for o in (-1, 1)]
    greeted += [ring("cols", n_cols, o) for o in (-1, 1)]
    greeted += [ring("cols", n_cols, o) for o in range(1, n_cols)]
    for device in greeted:
        pl.semaphore_signal(barrier, inc=1, device_id=device, device_id_type=MESH)

    groups = ((1, 1), (2, J - 2), (J, 1))

    def remote(src, dst, send, recv, device):
        return pltpu.make_async_remote_copy(
            src_ref=src, dst_ref=dst, send_sem=send, recv_sem=recv,
            device_id=device, device_id_type=MESH)

    def j_copy(side, b, src=None):
        mine, theirs = ((1, J + 1), (J, 0))[side]
        if src is None:
            src = X[b].at[mine, pl.ds(1, I), inner, :]
        return remote(src, X[b].at[theirs, pl.ds(1, I), inner, :],
                      js.at[side, b], jr.at[side, b], ring("rows", n_rows, (-1, 1)[side]))

    def i_copy(side, g, b):
        mine, theirs = ((1, I + 1), (I, 0))[side]
        first, size = groups[g]
        return remote(X[b].at[pl.ds(first, size), mine, inner, :],
                      X[b].at[pl.ds(first, size), theirs, inner, :],
                      is_.at[side, g, b], ir.at[side, g, b], ring("cols", n_cols, (-1, 1)[side]))

    def k_copy(side, g, b):
        first, size = groups[g]
        return remote(KS.at[b, side, pl.ds(first - 1, size)],
                      KR.at[b, 1 - side, pl.ds(first - 1, size)],
                      ks.at[side, g, b], kr.at[side, g, b], ring("slabs", n_slabs, (-1, 1)[side]))

    def t_copy(offset, g):
        first, size = groups[g]
        return remote(TS.at[pl.ds(first - 1, size)], TR.at[offset - 1, pl.ds(first - 1, size)],
                      ts.at[offset - 1, g], tr.at[offset - 1, g], ring("cols", n_cols, offset))

    ik = lambda g, b: [k_copy(s, g, b) for s in (0, 1)] + [i_copy(s, g, b) for s in (0, 1)]

    def over(g, body):
        first, size = groups[g]

        def at(n, carry):
            for i in range(1, I + 1):
                body(first + n, i)
            return carry

        lax.fori_loop(0, size, at, 0)

    def pack(b, j, i, low, high):
        KS[b, 0, j - 1, pl.ds(i - 1, 1), :] = low
        KS[b, 1, j - 1, pl.ds(i - 1, 1), :] = high

    def update(b, g, last):
        nb = 1 - b

        def unpack(j, i):
            X[b][j, i, PAD - 1:PAD, :] = KR[b, 0, j - 1, pl.ds(i - 1, 1), :]
            X[b][j, i, PAD + K:PAD + K + 1, :] = KR[b, 1, j - 1, pl.ds(i - 1, 1), :]

        over(g, unpack)

        def cell(j, i):
            c = X[b][j, i, PAD:PAD + K, :]
            around = X[b][j, i, PAD - 1:PAD + K - 1, :] + X[b][j, i, PAD + 1:PAD + K + 1, :]
            around += X[b][j - 1, i, PAD:PAD + K, :] + X[b][j + 1, i, PAD:PAD + K, :]
            around += X[b][j, i - 1, PAD:PAD + K, :] + X[b][j, i + 1, PAD:PAD + K, :]
            c2 = c * 0.2
            new = 0.1 * around + (c * 0.4 + c2 * (1.0 - c * C[j - 1, i - 1]))
            if last:
                end[j - 1, i - 1] = new
            else:
                X[nb][j, i, PAD:PAD + K, :] = new
                pack(nb, j, i, new[:1], new[K - 1:])

        over(g, cell)

    load_d.wait()
    for g in range(3):
        over(g, lambda j, i: pack(0, j, i, X0[j, i, PAD:PAD + 1, :], X0[j, i, PAD + K - 1:PAD + K, :]))
    pl.semaphore_wait(barrier, len(greeted))
    sent, sent_j = {}, {}
    for g in (1, 0, 2):
        sent[0, g] = ik(g, 0)
        for copy in sent[0, g]:
            copy.start()
    for side in (0, 1):
        sent_j[0, side] = j_copy(side, 0, (dens.at[0], dens.at[J - 1])[side])
    sent_j[0, 0].start()
    load_c.wait()

    me = lax.axis_index("cols")
    totals = []
    for t in range(STEPS):
        b, nb, last = t % 2, 1 - t % 2, t == STEPS - 1
        for g in (1, 0, 2):
            for copy in sent[t, g]:
                copy.wait_recv()
            if g != 1:
                sent_j[t, 1 - g // 2].wait_recv()
            if t >= 1:
                for copy in sent[t - 1, g]:
                    copy.wait_send()
                if g != 1:
                    sent_j[t - 1, g // 2].wait_send()
            update(b, g, last)
            if not last:
                sent[t + 1, g] = ik(g, nb)
                for copy in sent[t + 1, g]:
                    copy.start()
                if g != 1:
                    sent_j[t + 1, g // 2] = j_copy(g // 2, nb)
            if g == 1:
                sent_j[t, 1].start()
            elif g == 0 and not last:
                sent_j[t + 1, 0].start()
            if not last:
                continue
            first, size = groups[g]

            def total(n, carry, first=first):
                j = first + n
                so_far = end[j - 1, 0]
                for i in range(1, I):
                    so_far += end[j - 1, i]
                TS[j - 1] = so_far
                return carry

            lax.fori_loop(0, size, total, 0)
            copies = [t_copy(o, g) for o in range(1, n_cols)]
            for copy in copies:
                copy.start()
            totals.append((g, copies))
    for g, copies in totals:
        first, size = groups[g]
        for copy in copies:
            copy.wait()

        def gather(n, carry, first=first):
            j = first + n
            so_far = jnp.zeros((K, S), jnp.float32)
            for o in range(1, n_cols):
                so_far += jnp.where(o <= me, TR[o - 1, j - 1], 0.0)
            below[j - 1] = so_far
            return carry

        lax.fori_loop(0, size, gather, 0)
    for g in range(3):
        for copy in sent[STEPS - 1, g]:
            copy.wait_send()
    for side in range(2):
        sent_j[STEPS - 1, side].wait_send()


def write_out(cells, end, below, pot_out, end_out, PT, sems):
    J, I, K, S = end.shape
    parts = 4 if J % 4 == 0 else 1
    size = J // parts
    writes = []
    for p in range(parts):
        here = pl.ds(p * size, size)
        writes.append(pltpu.make_async_copy(end.at[here], end_out.at[here], sems.at[0, p]))
        writes[-1].start()
    for p in range(parts):
        def running(n, carry, p=p):
            j = p * size + n
            so_far = below[j]
            for i in range(I):
                so_far += end[j, i]
                PT[j, i] = so_far * (1.0 / cells)
            return carry

        lax.fori_loop(0, size, running, 0)
        here = pl.ds(p * size, size)
        writes.append(pltpu.make_async_copy(PT.at[here], pot_out.at[here], sems.at[1, p]))
        writes[-1].start()
    for write in writes:
        write.wait()


def solution(mesh):
    counts = tuple(mesh.shape[axis] for axis in ("rows", "cols", "slabs"))

    def per_device(density, crowding):
        J, I, K, S = density.shape
        n_cols = counts[1]
        any_space = pl.BlockSpec(memory_space=pl.ANY)
        dma = pltpu.SemaphoreType.DMA
        vmem = pl.BlockSpec(memory_space=pltpu.VMEM)
        padded = pltpu.VMEM((J + 2, I + 2, K + 2 * PAD, S), jnp.float32)
        end, below = pl.pallas_call(
            functools.partial(kernel, density.shape, counts),
            out_shape=[jax.ShapeDtypeStruct((J, I, K, S), jnp.float32),
                       jax.ShapeDtypeStruct((J, K, S), jnp.float32)],
            in_specs=[any_space] * 2,
            out_specs=[vmem] * 2,
            scratch_shapes=[
                padded, padded,
                pltpu.VMEM((J, I, K, S), jnp.float32),
                pltpu.VMEM((2, 2, J, I, S), jnp.float32),
                pltpu.VMEM((2, 2, J, I, S), jnp.float32),
                pltpu.VMEM((J, K, S), jnp.float32),
                pltpu.VMEM((n_cols - 1, J, K, S), jnp.float32),
                dma((2, 2)), dma((2, 2)),
                dma((2, 3, 2)), dma((2, 3, 2)),
                dma((2, 3, 2)), dma((2, 3, 2)),
                dma((n_cols - 1, 3)), dma((n_cols - 1, 3)),
                dma((2,)),
            ],
            compiler_params=pltpu.CompilerParams(
                collective_id=0, has_side_effects=True, vmem_limit_bytes=VMEM_FIRST),
            name="reaction_diffusion",
        )(density, crowding)
        return pl.pallas_call(
            functools.partial(write_out, I * n_cols),
            out_shape=[jax.ShapeDtypeStruct(density.shape, density.dtype)] * 2,
            in_specs=[vmem] * 2,
            out_specs=[any_space] * 2,
            scratch_shapes=[pltpu.VMEM((J, I, K, S), jnp.float32), dma((2, 4))],
            compiler_params=pltpu.CompilerParams(vmem_limit_bytes=VMEM_SECOND),
            name="write_out",
        )(end, below)

    spec = P(("copy", "rows"), "cols", "slabs", None)
    return jax.shard_map(
        per_device, mesh=mesh, in_specs=(spec, spec), out_specs=(spec, spec), check_vma=False)
```

```python
import functools

import jax
import jax.numpy as jnp
from jax import lax
from jax.experimental import pallas as pl
from jax.experimental.pallas import tpu as pltpu
from jax.sharding import PartitionSpec as P

STEPS = 6
MESH = pl.DeviceIdType.MESH
VMEM_FIRST = 47 * 2**20
VMEM_SECOND = 20 * 2**20
PAD = 8


def kernel(shape, counts, dens, crow, end, below, X0, X1, C, KS, KR, TS, TR,
           js, jr, is_, ir, ks, kr, ts, tr, ls):
    J, I, K, S = shape
    n_rows, n_cols, n_slabs = counts
    X = (X0, X1)
    inner = pl.ds(PAD, K)

    def ring(axis, count, offset):
        return {axis: lax.rem(lax.axis_index(axis) + (offset + count), count)}

    load_d = pltpu.make_async_copy(dens, X0.at[pl.ds(1, J), pl.ds(1, I), inner, :], ls.at[0])
    load_c = pltpu.make_async_copy(crow, C, ls.at[1])
    load_d.start()

    barrier = pltpu.get_barrier_semaphore()
    greeted = [ring("rows", n_rows, o) for o in (-1, 1)]
    greeted += [ring("slabs", n_slabs, o) for o in (-1, 1)]
    greeted += [ring("cols", n_cols, o) for o in (-1, 1)]
    greeted += [ring("cols", n_cols, o) for o in range(1, n_cols)]
    for device in greeted:
        pl.semaphore_signal(barrier, inc=1, device_id=device, device_id_type=MESH)

    groups = ((1, 1), (2, J - 2), (J, 1))

    def remote(src, dst, send, recv, device):
        return pltpu.make_async_remote_copy(
            src_ref=src, dst_ref=dst, send_sem=send, recv_sem=recv,
            device_id=device, device_id_type=MESH)

    def j_copy(side, b):
        mine, theirs = ((1, J + 1), (J, 0))[side]
        return remote(X[b].at[mine, pl.ds(1, I), inner, :], X[b].at[theirs, pl.ds(1, I), inner, :],
                      js.at[side, b], jr.at[side, b], ring("rows", n_rows, (-1, 1)[side]))

    def i_copy(side, g, b):
        mine, theirs = ((1, I + 1), (I, 0))[side]
        first, size = groups[g]
        return remote(X[b].at[pl.ds(first, size), mine, inner, :],
                      X[b].at[pl.ds(first, size), theirs, inner, :],
                      is_.at[side, g, b], ir.at[side, g, b], ring("cols", n_cols, (-1, 1)[side]))

    def k_copy(side, g, b):
        first, size = groups[g]
        return remote(KS.at[b, side, pl.ds(first - 1, size)],
                      KR.at[b, 1 - side, pl.ds(first - 1, size)],
                      ks.at[side, g, b], kr.at[side, g, b], ring("slabs", n_slabs, (-1, 1)[side]))

    def t_copy(offset, g):
        first, size = groups[g]
        return remote(TS.at[pl.ds(first - 1, size)], TR.at[offset - 1, pl.ds(first - 1, size)],
                      ts.at[offset - 1, g], tr.at[offset - 1, g], ring("cols", n_cols, offset))

    ik = lambda g, b: [k_copy(s, g, b) for s in (0, 1)] + [i_copy(s, g, b) for s in (0, 1)]

    def over(g, body):
        first, size = groups[g]

        def at(n, carry):
            for i in range(1, I + 1):
                body(first + n, i)
            return carry

        lax.fori_loop(0, size, at, 0)

    def pack(b, j, i, low, high):
        KS[b, 0, j - 1, pl.ds(i - 1, 1), :] = low
        KS[b, 1, j - 1, pl.ds(i - 1, 1), :] = high

    def unpack(b, g):
        def cell(j, i):
            X[b][j, i, PAD - 1:PAD, :] = KR[b, 0, j - 1, pl.ds(i - 1, 1), :]
            X[b][j, i, PAD + K:PAD + K + 1, :] = KR[b, 1, j - 1, pl.ds(i - 1, 1), :]

        over(g, cell)

    def update(b, g, last):
        nb = 1 - b

        def cell(j, i):
            c = X[b][j, i, PAD:PAD + K, :]
            around = X[b][j, i, PAD - 1:PAD + K - 1, :] + X[b][j, i, PAD + 1:PAD + K + 1, :]
            around += X[b][j - 1, i, PAD:PAD + K, :] + X[b][j + 1, i, PAD:PAD + K, :]
            around += X[b][j, i - 1, PAD:PAD + K, :] + X[b][j, i + 1, PAD:PAD + K, :]
            c2 = c * 0.2
            new = 0.1 * around + (c * 0.4 + c2 * (1.0 - c * C[j - 1, i - 1]))
            if last:
                end[j - 1, i - 1] = new
            else:
                X[nb][j, i, PAD:PAD + K, :] = new
                pack(nb, j, i, new[:1], new[K - 1:])

        over(g, cell)

    load_d.wait()
    load_c.start()
    for g in range(3):
        over(g, lambda j, i: pack(0, j, i, X0[j, i, PAD:PAD + 1, :], X0[j, i, PAD + K - 1:PAD + K, :]))
    pl.semaphore_wait(barrier, len(greeted))
    sent, sent_j = {}, {}
    for side in (0, 1):
        sent_j[0, side] = j_copy(side, 0)
    for g in (1, 0, 2):
        sent[0, g] = ik(g, 0)
        for copy in sent[0, g][:2]:
            copy.start()
    sent_j[0, 0].start()
    for g in (1, 0, 2):
        for copy in sent[0, g][2:]:
            copy.start()
    load_c.wait()

    me = lax.axis_index("cols")
    totals = []

    def collect(g, copies):
        first, size = groups[g]
        for copy in copies:
            copy.wait()

        def gather(n, carry):
            j = first + n
            so_far = jnp.zeros((K, S), jnp.float32)
            for o in range(1, n_cols):
                so_far += jnp.where(o <= me, TR[o - 1, j - 1], 0.0)
            below[j - 1] = so_far
            return carry

        lax.fori_loop(0, size, gather, 0)

    for t in range(STEPS):
        b, nb, last = t % 2, 1 - t % 2, t == STEPS - 1
        for g in (1, 0, 2):
            for copy in sent[t, g]:
                copy.wait_recv()
            unpack(b, g)
            if last and g == 2:
                for earlier in totals:
                    collect(*earlier)
            if g != 1:
                sent_j[t, 1 - g // 2].wait_recv()
            if t >= 1:
                for copy in sent[t - 1, g]:
                    copy.wait_send()
                if g != 1:
                    sent_j[t - 1, g // 2].wait_send()
            update(b, g, last)
            if not last:
                sent[t + 1, g] = ik(g, nb)
                for copy in sent[t + 1, g]:
                    copy.start()
                if g != 1:
                    sent_j[t + 1, g // 2] = j_copy(g // 2, nb)
            if g == 1:
                sent_j[t, 1].start()
            elif g == 0 and not last:
                sent_j[t + 1, 0].start()
            if not last:
                continue
            first, size = groups[g]

            def total(n, carry, first=first):
                j = first + n
                so_far = end[j - 1, 0]
                for i in range(1, I):
                    so_far += end[j - 1, i]
                TS[j - 1] = so_far
                return carry

            lax.fori_loop(0, size, total, 0)
            copies = [t_copy(o, g) for o in range(1, n_cols)]
            for copy in copies:
                copy.start()
            totals.append((g, copies))
    collect(*totals[2])
    for g in range(3):
        for copy in sent[STEPS - 1, g]:
            copy.wait_send()
    for side in range(2):
        sent_j[STEPS - 1, side].wait_send()


def write_out(cells, end, below, pot_out, end_out, PT, sems):
    J, I, K, S = end.shape
    parts = 4 if J % 4 == 0 else 1
    size = J // parts
    writes = []
    for p in range(parts):
        here = pl.ds(p * size, size)
        writes.append(pltpu.make_async_copy(end.at[here], end_out.at[here], sems.at[0, p]))
        writes[-1].start()
    for p in range(parts):
        def running(n, carry, p=p):
            j = p * size + n
            so_far = below[j]
            for i in range(I):
                so_far += end[j, i]
                PT[j, i] = so_far * (1.0 / cells)
            return carry

        lax.fori_loop(0, size, running, 0)
        here = pl.ds(p * size, size)
        writes.append(pltpu.make_async_copy(PT.at[here], pot_out.at[here], sems.at[1, p]))
        writes[-1].start()
    for write in writes:
        write.wait()


def solution(mesh):
    counts = tuple(mesh.shape[axis] for axis in ("rows", "cols", "slabs"))

    def per_device(density, crowding):
        J, I, K, S = density.shape
        n_cols = counts[1]
        any_space = pl.BlockSpec(memory_space=pl.ANY)
        dma = pltpu.SemaphoreType.DMA
        vmem = pl.BlockSpec(memory_space=pltpu.VMEM)
        padded = pltpu.VMEM((J + 2, I + 2, K + 2 * PAD, S), jnp.float32)
        end, below = pl.pallas_call(
            functools.partial(kernel, density.shape, counts),
            out_shape=[jax.ShapeDtypeStruct((J, I, K, S), jnp.float32),
                       jax.ShapeDtypeStruct((J, K, S), jnp.float32)],
            in_specs=[any_space] * 2,
            out_specs=[vmem] * 2,
            scratch_shapes=[
                padded, padded,
                pltpu.VMEM((J, I, K, S), jnp.float32),
                pltpu.VMEM((2, 2, J, I, S), jnp.float32),
                pltpu.VMEM((2, 2, J, I, S), jnp.float32),
                pltpu.VMEM((J, K, S), jnp.float32),
                pltpu.VMEM((n_cols - 1, J, K, S), jnp.float32),
                dma((2, 2)), dma((2, 2)),
                dma((2, 3, 2)), dma((2, 3, 2)),
                dma((2, 3, 2)), dma((2, 3, 2)),
                dma((n_cols - 1, 3)), dma((n_cols - 1, 3)),
                dma((2,)),
            ],
            compiler_params=pltpu.CompilerParams(
                collective_id=0, has_side_effects=True, vmem_limit_bytes=VMEM_FIRST),
            name="reaction_diffusion",
        )(density, crowding)
        return pl.pallas_call(
            functools.partial(write_out, I * n_cols),
            out_shape=[jax.ShapeDtypeStruct(density.shape, density.dtype)] * 2,
            in_specs=[vmem] * 2,
            out_specs=[any_space] * 2,
            scratch_shapes=[pltpu.VMEM((J, I, K, S), jnp.float32), dma((2, 4))],
            compiler_params=pltpu.CompilerParams(vmem_limit_bytes=VMEM_SECOND),
            name="write_out",
        )(end, below)

    spec = P(("copy", "rows"), "cols", "slabs", None)
    return jax.shard_map(
        per_device, mesh=mesh, in_specs=(spec, spec), out_specs=(spec, spec), check_vma=False)
```
